256 devices in a mesh: row: 8 (over y, z_hi), col: 32 (over z_lo, x, core).
Axes of the slice: x: 4, y: 4, z: 8 (z_hi: 2, z_lo: 4; z = z_hi * 4 + z_lo), core: 2. Of those that a mesh axis runs over, the one named last changes fastest.
Arguments:
- g_greater: bfloat16 [256, 256, 2, 4096], P('row', 'col'), may hold values from -6 to 6
- g_lesser: bfloat16 [256, 256, 2, 4096], P('row', 'col'), may hold values from -6 to 6
- coupling: float32 [64, 64], replicated, may hold values from 0.5 to 1.5
- partner: int32 [64], replicated, may hold values from 0 to 63, each once
- memory_start: int32 [256], P('row'), may hold values from 0 to 255, as said below
Outputs:
- collision: bfloat16 [256, 4, 2, 4096], P(('row', 'col'))
The draws below stay inside these ranges and needn't reach their ends.
Inputs may be any that keep to these rules, and one draw needn't show every extreme that they name: partner names every orbital once. memory_start[t] lies between 0 and t.
All inputs are finite; a program needn't handle non-finite values.
Results may differ from the reference program's by a relative error of at most 0.0049.
Values may be sent and summed in bfloat16 or wider, within the bound.
No kernel may reach another device: no remote copies, remote signals or barrier semaphores. Data moves between devices by JAX's collectives and lax.ppermute only.
A program may use at most 192 MiB of HBM per device.

```python
import math
import jax
import jax.numpy as jnp
from jax import lax

ORB = 64
TW = 4
SPAN = 32
TC = 8
NT = 256
CYCLE = 32
N_ROW = 8


def draw_memory_start(key, part):
    time_ids = jnp.arange(NT, dtype=jnp.int32)
    drawn = jax.random.randint(key, (NT,), 0, time_ids + 1).astype(jnp.int32)
    return jnp.where(time_ids == NT - 1, time_ids, drawn).astype(jnp.int32)


def shard_levels(key, extent, split, smallest, high):
    def one(dim, blocks):
        draws = jax.random.uniform(jax.random.fold_in(jax.random.fold_in(key, 6), dim), (blocks,), jnp.float32, smallest / len(split), high / len(split))
        return jnp.repeat(jnp.exp(draws), extent[dim] // blocks).reshape((-1,) + (1,) * (len(extent) - dim - 1))

    gain = one(*split[0])
    for cut in split[1:]:
        gain = gain * one(*cut)
    return gain


def noise(stream_key, shape, deviation, reach, shards=(), kind=jnp.bfloat16):
    values = deviation * jax.random.normal(stream_key, shape, jnp.float32)
    if shards:
        values = values * shard_levels(stream_key, shape, shards, -0.22, 0.18)
    return jnp.clip(values, -reach, reach).astype(kind)


def setup_inputs(seed: int = 0) -> dict:
    keys = jax.random.split(jax.random.key(seed), 6)
    g_greater = noise(keys[0], (NT, NT, 2, ORB * ORB), 1.0, 6.0, ((0, 8), (1, 32)))
    g_lesser = noise(keys[1], (NT, NT, 2, ORB * ORB), 1.0, 6.0, ((0, 8), (1, 32)))
    coupling = jnp.clip(jax.random.uniform(keys[2], (ORB, ORB), jnp.float32, 0.5, 1.5), 0.5, 1.5)
    partner = jax.random.permutation(keys[3], ORB).astype(jnp.int32)
    memory_start = draw_memory_start(jax.random.fold_in(keys[5], 71), 0)
    return {"g_greater": g_greater, "g_lesser": g_lesser, "coupling": coupling, "partner": partner, "memory_start": memory_start}


def complex_product(left_real, left_imag, right_real, right_imag):
    return (left_real * right_real - left_imag * right_imag, left_real * right_imag + left_imag * right_real)

def self_energy(direct, partnered, mirrored, weight):
    first_pair = complex_product(direct[0], direct[1], partnered[0], partnered[1])
    triple = complex_product(first_pair[0], first_pair[1], mirrored[0], mirrored[1])
    return (weight * triple[0], weight * triple[1])

def split_parts(array):
    return (array[:, 0].astype(jnp.float32), array[:, 1].astype(jnp.float32))

def reference(g_greater, g_lesser, coupling, partner, memory_start):
    pair_count = ORB * ORB
    orbit_ids = jnp.arange(ORB, dtype=jnp.int32)
    permuted = (partner[:, None] * ORB + partner[None, :]).reshape(pair_count).astype(jnp.int32)
    flipped = (orbit_ids[None, :] * ORB + orbit_ids[:, None]).reshape(pair_count).astype(jnp.int32)
    weight = coupling.reshape(pair_count).astype(jnp.float32)
    time_ids = jnp.arange(NT, dtype=jnp.int32)
    stored = (time_ids % CYCLE * TC + time_ids // CYCLE).astype(jnp.int32)
    scaling = 1.0 / (4.0 * math.sqrt(ORB * NT))

    def one_block(block):
        offsets = (block * SPAN + jnp.arange(TW, dtype=jnp.int32)).astype(jnp.int32)
        lesser_slab = jnp.take(g_lesser, stored[offsets], axis=1)
        lesser_slab = lesser_slab.reshape(NT, TW, 2, ORB, ORB).astype(jnp.float32)
        slab_real = lesser_slab[:, :, 0]
        slab_imag = lesser_slab[:, :, 1]

        def one_time(moment):
            row_greater = jnp.take(lax.dynamic_index_in_dim(g_greater, moment, 0, False), stored, axis=0)
            row_lesser = jnp.take(lax.dynamic_index_in_dim(g_lesser, moment, 0, False), stored, axis=0)
            stored_col = stored[moment]
            back_greater = lax.dynamic_index_in_dim(g_greater, stored_col, 1, False)
            back_lesser = lax.dynamic_index_in_dim(g_lesser, stored_col, 1, False)
            greater_sig = self_energy(split_parts(row_greater), split_parts(jnp.take(row_greater, permuted, axis=2)), split_parts(jnp.take(back_lesser, flipped, axis=2)), weight)
            lesser_sig = self_energy(split_parts(row_lesser), split_parts(jnp.take(row_lesser, permuted, axis=2)), split_parts(jnp.take(back_greater, flipped, axis=2)), weight)
            live_mask = ((time_ids >= memory_start[moment]) & (time_ids <= moment))[:, None]
            ret_real = jnp.where(live_mask, greater_sig[0] - lesser_sig[0], 0.0)
            ret_imag = jnp.where(live_mask, greater_sig[1] - lesser_sig[1], 0.0)
            ret_real = lax.optimization_barrier(ret_real.astype(jnp.bfloat16)).astype(jnp.float32).reshape(NT, ORB, ORB)
            ret_imag = lax.optimization_barrier(ret_imag.astype(jnp.bfloat16)).astype(jnp.float32).reshape(NT, ORB, ORB)
            out_real = jnp.einsum('sik,swkl->wil', ret_real, slab_real) - jnp.einsum('sik,swkl->wil', ret_imag, slab_imag)
            out_imag = jnp.einsum('sik,swkl->wil', ret_real, slab_imag) + jnp.einsum('sik,swkl->wil', ret_imag, slab_real)
            joined = jnp.stack([out_real, out_imag], axis=1) * scaling
            return joined.reshape(TW, 2, pair_count).astype(jnp.bfloat16)
        return lax.map(one_time, (block * SPAN + jnp.arange(SPAN, dtype=jnp.int32)).astype(jnp.int32))
    result = lax.map(one_block, jnp.arange(N_ROW, dtype=jnp.int32))
    return result.reshape(NT, TW, 2, pair_count)
```

```python
import math

import jax
import jax.numpy as jnp
from jax import lax
from jax.experimental import pallas as pl
from jax.experimental.pallas import tpu as pltpu
from jax.sharding import PartitionSpec as P

TW = 4
ORB = 64
PAIRS = 32
LANES = 128
GROUP = 4


def tile_view(array):
    rows, cols, comps, pairs = array.shape
    split = array.reshape(rows, cols, comps, pairs // LANES, LANES)
    return split.transpose(0, 1, 3, 2, 4).reshape(rows * cols, comps * (pairs // LANES), LANES)


def direct_kernel(tiles_ref, swap_ref, move_ref, move_perm_ref, weight_ref, out_ref, flat, turned, turned_perm, stage, stage_perm):
    tiles = tiles_ref.shape[0]
    groups = tiles // GROUP
    flat[...] = tiles_ref[...].reshape(tiles * 2 * PAIRS, LANES).astype(jnp.float32)

    def one_group(index, carry):
        for comp in range(2):
            base = index * (GROUP * 2 * PAIRS) + comp
            block = flat[pl.ds(base, GROUP * PAIRS, stride=2), :]
            swapped = jnp.dot(
                block.astype(jnp.bfloat16), swap_ref[...], preferred_element_type=jnp.float32
            )
            turned[...] = block.T
            turned_perm[...] = swapped.T
            row = pl.multiple_of(index * (2 * PAIRS) + comp * PAIRS, PAIRS)
            for part in range(4):
                start = (part // 2) * ORB + part % 2
                cols = slice(part * LANES, (part + 1) * LANES)
                stage[pl.ds(row, PAIRS), cols] = turned[pl.ds(start, PAIRS, stride=2), :].astype(
                    jnp.bfloat16
                )
                stage_perm[pl.ds(row, PAIRS), cols] = turned_perm[
                    pl.ds(start, PAIRS, stride=2), :
                ].astype(jnp.bfloat16)
        return carry

    lax.fori_loop(0, groups, one_group, 0)
    weight = weight_ref[...]

    def one_product(index, carry):
        row = pl.multiple_of(index * (2 * PAIRS), 2 * PAIRS)
        plain = jnp.dot(
            stage[pl.ds(row, 2 * PAIRS), :], move_ref[...], preferred_element_type=jnp.float32
        )
        moved = jnp.dot(
            stage_perm[pl.ds(row, 2 * PAIRS), :],
            move_perm_ref[...],
            preferred_element_type=jnp.float32,
        )
        for item in range(GROUP):
            cols = slice(item * LANES, (item + 1) * LANES)
            a_real = plain[:PAIRS, cols]
            a_imag = plain[PAIRS:, cols]
            b_real = moved[:PAIRS, cols]
            b_imag = moved[PAIRS:, cols]
            out_ref[index * GROUP + item, 0] = weight * (a_real * b_real - a_imag * b_imag)
            out_ref[index * GROUP + item, 1] = weight * (a_real * b_imag + a_imag * b_real)
        return carry

    lax.fori_loop(0, groups, one_product, 0)


def direct_part(tiles, swap, move, move_perm, weight, block=32):
    count = tiles.shape[0]
    return pl.pallas_call(
        direct_kernel,
        grid=(count // block,),
        in_specs=[
            pl.BlockSpec((block, 2 * PAIRS, LANES), lambda n: (n, 0, 0)),
            pl.BlockSpec(swap.shape, lambda n: (0, 0)),
            pl.BlockSpec(move.shape, lambda n: (0, 0)),
            pl.BlockSpec(move_perm.shape, lambda n: (0, 0)),
            pl.BlockSpec(weight.shape, lambda n: (0, 0)),
        ],
        out_specs=pl.BlockSpec((block, 2, PAIRS, LANES), lambda n: (n, 0, 0, 0)),
        out_shape=jax.ShapeDtypeStruct((count, 2, PAIRS, LANES), jnp.float32),
        scratch_shapes=[
            pltpu.VMEM((block * 2 * PAIRS, LANES), jnp.float32),
            pltpu.VMEM((LANES, LANES), jnp.float32),
            pltpu.VMEM((LANES, LANES), jnp.float32),
            pltpu.VMEM((block // GROUP * 2 * PAIRS, GROUP * LANES), jnp.bfloat16),
            pltpu.VMEM((block // GROUP * 2 * PAIRS, GROUP * LANES), jnp.bfloat16),
        ],
        cost_estimate=pl.CostEstimate(
            flops=count * 64 * 512 * 512, bytes_accessed=count * 49152, transcendentals=0
        ),
        name="direct_part",
    )(tiles, swap, move, move_perm, weight)


def mirror_kernel(direct_ref, tiles_ref, out_ref, flat):
    tiles = tiles_ref.shape[0]
    flat[...] = tiles_ref[...].reshape(tiles * 2 * PAIRS, LANES).astype(jnp.float32)

    def one_tile(index, carry):
        m_real = flat[pl.ds(index * 2 * PAIRS, PAIRS, stride=2), :]
        m_imag = flat[pl.ds(index * 2 * PAIRS + 1, PAIRS, stride=2), :]
        d_real = direct_ref[index, 0]
        d_imag = direct_ref[index, 1]
        out_ref[index, 0] = d_real * m_real - d_imag * m_imag
        out_ref[index, 1] = d_real * m_imag + d_imag * m_real
        return carry

    lax.fori_loop(0, tiles, one_tile, 0, unroll=4)


def mirror_part(direct, tiles, block=32):
    count = tiles.shape[0]
    full = pl.BlockSpec((block, 2, PAIRS, LANES), lambda n: (n, 0, 0, 0))
    return pl.pallas_call(
        mirror_kernel,
        grid=(count // block,),
        in_specs=[full, pl.BlockSpec((block, 2 * PAIRS, LANES), lambda n: (n, 0, 0))],
        out_specs=full,
        out_shape=jax.ShapeDtypeStruct(direct.shape, jnp.float32),
        scratch_shapes=[pltpu.VMEM((block * 2 * PAIRS, LANES), jnp.float32)],
        cost_estimate=pl.CostEstimate(
            flops=count * 65536, bytes_accessed=count * 81920, transcendentals=0
        ),
        name="mirror_part",
    )(direct, tiles)


def integral_kernel(live_ref, first_ref, direct_ref, tiles_ref, slab_ref, out_ref, flat, right):
    tiles = tiles_ref.shape[0]
    steps = tiles // out_ref.shape[0]
    step = pl.program_id(0)
    flat[...] = tiles_ref[...].reshape(tiles * 2 * PAIRS, LANES).astype(jnp.float32)
    for moment in range(out_ref.shape[0]):
        cols = slice(moment * LANES, (moment + 1) * LANES)
        for item in range(steps):
            index = moment * steps + item
            live = live_ref[step * tiles + index] > 0
            m_real = flat[pl.ds(index * 2 * PAIRS, PAIRS, stride=2), :]
            m_imag = flat[pl.ds(index * 2 * PAIRS + 1, PAIRS, stride=2), :]
            d_real = direct_ref[index, 0]
            d_imag = direct_ref[index, 1]
            ret_real = first_ref[index, 0] - (d_real * m_real - d_imag * m_imag)
            ret_imag = first_ref[index, 1] - (d_real * m_imag + d_imag * m_real)
            row = item * 2 * PAIRS
            right[row : row + PAIRS, cols] = jnp.where(live, ret_real, 0.0).astype(jnp.bfloat16)
            right[row + PAIRS : row + 2 * PAIRS, cols] = jnp.where(live, ret_imag, 0.0).astype(
                jnp.bfloat16
            )
    product = jnp.dot(slab_ref[...], right[...], preferred_element_type=jnp.float32)
    quarter = product.shape[0] // 4
    lower = lax.broadcasted_iota(jnp.int32, (quarter, LANES), 1) < ORB
    for moment in range(out_ref.shape[0]):
        cols = slice(moment * LANES, (moment + 1) * LANES)
        even_real = product[:quarter, cols]
        even_imag = product[quarter : 2 * quarter, cols]
        odd_real = product[2 * quarter : 3 * quarter, cols]
        odd_imag = product[3 * quarter :, cols]
        kept = jnp.where(lower, even_real, odd_imag)
        crossed = jnp.where(lower, even_imag, odd_real)
        out_ref[moment] = (kept + pltpu.roll(crossed, ORB, 1)).astype(out_ref.dtype)


def integral_part(live, first, direct, tiles, slab, moments=2):
    count = tiles.shape[0]
    rows = live.shape[0] // 8
    block = count // rows * moments
    full = pl.BlockSpec((block, 2, PAIRS, LANES), lambda n: (n, 0, 0, 0))
    return pl.pallas_call(
        integral_kernel,
        grid=(rows // moments,),
        in_specs=[
            pl.BlockSpec(memory_space=pltpu.SMEM),
            full,
            full,
            pl.BlockSpec((block, 2 * PAIRS, LANES), lambda n: (n, 0, 0)),
            pl.BlockSpec(slab.shape, lambda n: (0, 0)),
        ],
        out_specs=pl.BlockSpec((moments, TW * ORB, LANES), lambda n: (n, 0, 0)),
        out_shape=jax.ShapeDtypeStruct((rows, TW * ORB, LANES), jnp.bfloat16),
        scratch_shapes=[
            pltpu.VMEM((block * 2 * PAIRS, LANES), jnp.float32),
            pltpu.VMEM((slab.shape[1], moments * LANES), jnp.bfloat16),
        ],
        cost_estimate=pl.CostEstimate(
            flops=rows * 2 * 1024 * 512 * 128, bytes_accessed=count * 81920, transcendentals=0
        ),
        name="integral_part",
    )(live, first, direct, tiles, slab)


def per_device(g_greater, g_lesser, coupling, partner, memory_start):
    tile_rows, tile_cols, components, pair_count = g_greater.shape
    row_count = lax.axis_size("row")
    col_count = lax.axis_size("col")
    orbits = coupling.shape[0]
    both = ("col", "row")
    tiles_greater = tile_view(g_greater)
    tiles_lesser = tile_view(g_lesser)
    flip_lesser = lax.all_to_all(tiles_lesser, both, 0, 0, tiled=True)
    flip_greater = lax.all_to_all(tiles_greater, both, 0, 0, tiled=True)

    orbit_ids = jnp.arange(orbits, dtype=jnp.int32)
    one_hot = (partner[:, None] == orbit_ids[None, :]).astype(jnp.bfloat16)
    swap = jnp.kron(jnp.eye(2, dtype=jnp.bfloat16), one_hot.T)
    source = jnp.arange(GROUP * LANES, dtype=jnp.int32)
    src_ib = source // (2 * LANES)
    src_jb = source // LANES % 2
    src_item = source % LANES // PAIRS
    src_orbit = source % PAIRS * 2 + src_ib
    dst_item = source // LANES
    dst_jb = source // ORB % 2
    dst_orbit = source % ORB
    same = (src_item[:, None] == dst_item[None, :]) & (src_jb[:, None] == dst_jb[None, :])
    move = (same & (src_orbit[:, None] == dst_orbit[None, :])).astype(jnp.bfloat16)
    wanted = jnp.tile(partner, 2 * GROUP)
    move_perm = (same & (src_orbit[:, None] == wanted[None, :])).astype(jnp.bfloat16)
    weight = coupling.T.reshape(PAIRS, LANES)

    direct_lesser = direct_part(tiles_lesser, swap, move, move_perm, weight)
    direct_greater = direct_part(tiles_greater, swap, move, move_perm, weight)
    first = mirror_part(direct_greater, flip_lesser)

    window = flip_lesser[: TW * tile_cols].reshape(TW, tile_cols, PAIRS, 2, 2, orbits)
    slab_real = window[:, :, :, 0]
    slab_imag = window[:, :, :, 1]
    to_real = jnp.stack([slab_real, -slab_imag], axis=0)
    to_imag = jnp.stack([slab_imag, slab_real], axis=0)
    slab = jnp.stack([to_real, to_imag], axis=0)
    slab = slab.transpose(5, 0, 2, 6, 3, 1, 4).reshape(
        2 * 2 * TW * orbits, tile_cols * 2 * PAIRS
    )
    first_times = lax.axis_index("row") * tile_rows + jnp.arange(tile_rows, dtype=jnp.int32)
    second_times = jnp.arange(tile_cols, dtype=jnp.int32) * col_count + lax.axis_index("col")
    live = (second_times[None, :] >= memory_start[:, None]) & (
        second_times[None, :] <= first_times[:, None]
    )
    live = live.astype(jnp.int32).reshape(tile_rows * tile_cols)
    partial = integral_part(live, first, direct_lesser, flip_greater, slab)
    shares = lax.all_to_all(partial, "col", 0, 0, tiled=True)
    scaling = 1.0 / (4.0 * math.sqrt(orbits * tile_rows * row_count))
    summed = shares.astype(jnp.float32).sum(axis=0) * scaling
    summed = summed.reshape(TW, orbits, 2, orbits).transpose(0, 2, 3, 1)
    return summed.reshape(1, TW, 2, pair_count).astype(jnp.bfloat16)


def solution(mesh):
    return jax.shard_map(
        per_device,
        mesh=mesh,
        in_specs=(P("row", "col", None, None), P("row", "col", None, None), P(), P(), P("row")),
        out_specs=P(("row", "col"), None, None, None),
        check_vma=False,
    )
```

```python
import math

import jax
import jax.numpy as jnp
from jax import lax
from jax.experimental import pallas as pl
from jax.experimental.pallas import tpu as pltpu
from jax.sharding import PartitionSpec as P

TW = 4
ORB = 64
PAIRS = 32
LANES = 128
GROUP = 4


def tile_view(array):
    rows, cols, comps, pairs = array.shape
    split = array.reshape(rows, cols, comps, pairs // LANES, LANES)
    return split.transpose(0, 1, 3, 2, 4).reshape(rows * cols, comps * (pairs // LANES), LANES)


def direct_kernel(tiles_ref, swap_ref, move_ref, move_perm_ref, weight_ref, out_ref, flat, turned, turned_perm, stage, stage_perm):
    tiles = tiles_ref.shape[0]
    groups = tiles // GROUP
    flat[...] = tiles_ref[...].reshape(tiles * 2 * PAIRS, LANES).astype(jnp.float32)

    def one_group(index, carry):
        for comp in range(2):
            base = index * (GROUP * 2 * PAIRS) + comp
            block = flat[pl.ds(base, GROUP * PAIRS, stride=2), :]
            swapped = jnp.dot(
                block.astype(jnp.bfloat16), swap_ref[...], preferred_element_type=jnp.float32
            )
            turned[...] = block.T
            turned_perm[...] = swapped.T
            row = pl.multiple_of(index * (2 * PAIRS) + comp * PAIRS, PAIRS)
            for part in range(4):
                start = (part // 2) * ORB + part % 2
                cols = slice(part * LANES, (part + 1) * LANES)
                stage[pl.ds(row, PAIRS), cols] = turned[pl.ds(start, PAIRS, stride=2), :].astype(
                    jnp.bfloat16
                )
                stage_perm[pl.ds(row, PAIRS), cols] = turned_perm[
                    pl.ds(start, PAIRS, stride=2), :
                ].astype(jnp.bfloat16)
        return carry

    lax.fori_loop(0, groups, one_group, 0)
    weight = weight_ref[...]

    def one_product(index, carry):
        row = pl.multiple_of(index * (2 * PAIRS), 2 * PAIRS)
        plain = jnp.dot(
            stage[pl.ds(row, 2 * PAIRS), :], move_ref[...], preferred_element_type=jnp.float32
        )
        moved = jnp.dot(
            stage_perm[pl.ds(row, 2 * PAIRS), :],
            move_perm_ref[...],
            preferred_element_type=jnp.float32,
        )
        for item in range(GROUP):
            cols = slice(item * LANES, (item + 1) * LANES)
            a_real = plain[:PAIRS, cols]
            a_imag = plain[PAIRS:, cols]
            b_real = moved[:PAIRS, cols]
            b_imag = moved[PAIRS:, cols]
            out_ref[index * GROUP + item, 0] = weight * (a_real * b_real - a_imag * b_imag)
            out_ref[index * GROUP + item, 1] = weight * (a_real * b_imag + a_imag * b_real)
        return carry

    lax.fori_loop(0, groups, one_product, 0)


def direct_part(tiles, swap, move, move_perm, weight, block=32):
    count = tiles.shape[0]
    return pl.pallas_call(
        direct_kernel,
        grid=(count // block,),
        in_specs=[
            pl.BlockSpec((block, 2 * PAIRS, LANES), lambda n: (n, 0, 0)),
            pl.BlockSpec(swap.shape, lambda n: (0, 0)),
            pl.BlockSpec(move.shape, lambda n: (0, 0)),
            pl.BlockSpec(move_perm.shape, lambda n: (0, 0)),
            pl.BlockSpec(weight.shape, lambda n: (0, 0)),
        ],
        out_specs=pl.BlockSpec((block, 2, PAIRS, LANES), lambda n: (n, 0, 0, 0)),
        out_shape=jax.ShapeDtypeStruct((count, 2, PAIRS, LANES), jnp.float32),
        scratch_shapes=[
            pltpu.VMEM((block * 2 * PAIRS, LANES), jnp.float32),
            pltpu.VMEM((LANES, LANES), jnp.float32),
            pltpu.VMEM((LANES, LANES), jnp.float32),
            pltpu.VMEM((block // GROUP * 2 * PAIRS, GROUP * LANES), jnp.bfloat16),
            pltpu.VMEM((block // GROUP * 2 * PAIRS, GROUP * LANES), jnp.bfloat16),
        ],
        cost_estimate=pl.CostEstimate(
            flops=count * 64 * 512 * 512, bytes_accessed=count * 49152, transcendentals=0
        ),
        name="direct_part",
    )(tiles, swap, move, move_perm, weight)


def mirror_kernel(direct_ref, tiles_ref, out_ref, flat):
    tiles = tiles_ref.shape[0]
    flat[...] = tiles_ref[...].reshape(tiles * 2 * PAIRS, LANES).astype(jnp.float32)

    def one_tile(index, carry):
        m_real = flat[pl.ds(index * 2 * PAIRS, PAIRS, stride=2), :]
        m_imag = flat[pl.ds(index * 2 * PAIRS + 1, PAIRS, stride=2), :]
        d_real = direct_ref[index, 0]
        d_imag = direct_ref[index, 1]
        out_ref[index, 0] = d_real * m_real - d_imag * m_imag
        out_ref[index, 1] = d_real * m_imag + d_imag * m_real
        return carry

    lax.fori_loop(0, tiles, one_tile, 0, unroll=4)


def mirror_part(direct, tiles, block=32):
    count = tiles.shape[0]
    full = pl.BlockSpec((block, 2, PAIRS, LANES), lambda n: (n, 0, 0, 0))
    return pl.pallas_call(
        mirror_kernel,
        grid=(count // block,),
        in_specs=[full, pl.BlockSpec((block, 2 * PAIRS, LANES), lambda n: (n, 0, 0))],
        out_specs=full,
        out_shape=jax.ShapeDtypeStruct(direct.shape, jnp.float32),
        scratch_shapes=[pltpu.VMEM((block * 2 * PAIRS, LANES), jnp.float32)],
        cost_estimate=pl.CostEstimate(
            flops=count * 65536, bytes_accessed=count * 81920, transcendentals=0
        ),
        name="mirror_part",
    )(direct, tiles)


def integral_kernel(parity_ref, live_ref, first_ref, direct_ref, tiles_ref, slab_ref, out_ref, flat, *rights):
    moments, steps = tiles_ref.shape[:2]
    pair = moments // len(rights)
    step = pl.program_id(0)
    flat[...] = tiles_ref[...].reshape(moments * steps * 2 * PAIRS, LANES).astype(jnp.float32)
    slab = slab_ref[...]
    quarter = slab.shape[0] // 4
    lower = lax.broadcasted_iota(jnp.int32, (quarter, LANES), 1) < ORB
    for half, right in enumerate(rights):
        for inner in range(pair):
            moment = half * pair + inner
            time = (step * moments + moment) * 2 + parity_ref[0]
            cols = slice(inner * LANES, (inner + 1) * LANES)
            for item in range(steps):
                live = live_ref[time * steps + item] > 0
                base = (moment * steps + item) * 2 * PAIRS
                m_real = flat[pl.ds(base, PAIRS, stride=2), :]
                m_imag = flat[pl.ds(base + 1, PAIRS, stride=2), :]
                d_real = direct_ref[moment, item, 0]
                d_imag = direct_ref[moment, item, 1]
                ret_real = first_ref[moment, item, 0] - (d_real * m_real - d_imag * m_imag)
                ret_imag = first_ref[moment, item, 1] - (d_real * m_imag + d_imag * m_real)
                row = item * 2 * PAIRS
                right[row : row + PAIRS, cols] = jnp.where(live, ret_real, 0.0).astype(
                    jnp.bfloat16
                )
                right[row + PAIRS : row + 2 * PAIRS, cols] = jnp.where(
                    live, ret_imag, 0.0
                ).astype(jnp.bfloat16)
        product = jnp.dot(slab, right[...], preferred_element_type=jnp.float32)
        for inner in range(pair):
            cols = slice(inner * LANES, (inner + 1) * LANES)
            even_real = product[:quarter, cols]
            even_imag = product[quarter : 2 * quarter, cols]
            odd_real = product[2 * quarter : 3 * quarter, cols]
            odd_imag = product[3 * quarter :, cols]
            kept = jnp.where(lower, even_real, odd_imag)
            crossed = jnp.where(lower, even_imag, odd_real)
            out_ref[half * pair + inner] = kept + pltpu.roll(crossed, ORB, 1)


def integral_part(parity, live, first, direct, tiles, slab, steps, moments=4, halves=2):
    rows = tiles.shape[0] // steps
    first = first.reshape(rows // 2, 2, steps, 2, PAIRS, LANES)
    direct = direct.reshape(rows // 2, 2, steps, 2, PAIRS, LANES)
    tiles = tiles.reshape(rows // 2, 2, steps, 2 * PAIRS, LANES)
    full = pl.BlockSpec(
        (moments, None, steps, 2, PAIRS, LANES), lambda n, p, v: (n, p[0], 0, 0, 0, 0)
    )
    return pl.pallas_call(
        integral_kernel,
        grid_spec=pltpu.PrefetchScalarGridSpec(
            num_scalar_prefetch=2,
            grid=(rows // 2 // moments,),
            in_specs=[
                full,
                full,
                pl.BlockSpec(
                    (moments, None, steps, 2 * PAIRS, LANES), lambda n, p, v: (n, p[0], 0, 0, 0)
                ),
                pl.BlockSpec(slab.shape, lambda n, p, v: (0, 0)),
            ],
            out_specs=pl.BlockSpec((moments, TW * ORB, LANES), lambda n, p, v: (n, 0, 0)),
            scratch_shapes=[pltpu.VMEM((moments * steps * 2 * PAIRS, LANES), jnp.float32)]
            + [pltpu.VMEM((slab.shape[1], moments // halves * LANES), jnp.bfloat16)] * halves,
        ),
        out_shape=jax.ShapeDtypeStruct((rows // 2, TW * ORB, LANES), jnp.float32),
        cost_estimate=pl.CostEstimate(
            flops=rows * 1024 * 512 * 128, bytes_accessed=rows * steps * 40960, transcendentals=0
        ),
        name="integral_part",
    )(parity, live, first, direct, tiles, slab)


def per_device(g_greater, g_lesser, coupling, partner, memory_start):
    tile_rows, tile_cols, components, pair_count = g_greater.shape
    row_count = lax.axis_size("row")
    col_count = lax.axis_size("col")
    orbits = coupling.shape[0]
    both = ("col", "row")
    tiles_greater = tile_view(g_greater)
    tiles_lesser = tile_view(g_lesser)
    flip_lesser = lax.all_to_all(tiles_lesser, both, 0, 0, tiled=True)

    orbit_ids = jnp.arange(orbits, dtype=jnp.int32)
    one_hot = (partner[:, None] == orbit_ids[None, :]).astype(jnp.bfloat16)
    swap = jnp.kron(jnp.eye(2, dtype=jnp.bfloat16), one_hot.T)
    source = jnp.arange(GROUP * LANES, dtype=jnp.int32)
    src_ib = source // (2 * LANES)
    src_jb = source // LANES % 2
    src_item = source % LANES // PAIRS
    src_orbit = source % PAIRS * 2 + src_ib
    dst_item = source // LANES
    dst_jb = source // ORB % 2
    dst_orbit = source % ORB
    same = (src_item[:, None] == dst_item[None, :]) & (src_jb[:, None] == dst_jb[None, :])
    move = (same & (src_orbit[:, None] == dst_orbit[None, :])).astype(jnp.bfloat16)
    wanted = jnp.tile(partner, 2 * GROUP)
    move_perm = (same & (src_orbit[:, None] == wanted[None, :])).astype(jnp.bfloat16)
    weight = coupling.T.reshape(PAIRS, LANES)

    direct_lesser = direct_part(tiles_lesser, swap, move, move_perm, weight)
    direct_greater = direct_part(tiles_greater, swap, move, move_perm, weight)
    tiles_greater, direct_lesser, direct_greater = lax.optimization_barrier(
        (tiles_greater, direct_lesser, direct_greater)
    )
    flip_greater = lax.all_to_all(tiles_greater, both, 0, 0, tiled=True)
    first = mirror_part(direct_greater, flip_lesser)

    window = flip_lesser[: TW * tile_cols].reshape(TW, tile_cols, PAIRS, 2, 2, orbits)
    slab_real = window[:, :, :, 0]
    slab_imag = window[:, :, :, 1]
    to_real = jnp.stack([slab_real, -slab_imag], axis=0)
    to_imag = jnp.stack([slab_imag, slab_real], axis=0)
    slab = jnp.stack([to_real, to_imag], axis=0)
    slab = slab.transpose(5, 0, 2, 6, 3, 1, 4).reshape(
        2 * 2 * TW * orbits, tile_cols * 2 * PAIRS
    )
    first_times = lax.axis_index("row") * tile_rows + jnp.arange(tile_rows, dtype=jnp.int32)
    second_times = jnp.arange(tile_cols, dtype=jnp.int32) * col_count + lax.axis_index("col")
    live = (second_times[None, :] >= memory_start[:, None]) & (
        second_times[None, :] <= first_times[:, None]
    )
    live = live.astype(jnp.int32).reshape(tile_rows * tile_cols)
    core = lax.axis_index("col") % 2
    away = integral_part(
        jnp.reshape(1 - core, (1,)), live, first, direct_lesser, flip_greater, slab, tile_cols
    )
    arrived = lax.ppermute(away, "col", [(item, item ^ 1) for item in range(col_count)])
    kept = integral_part(
        jnp.reshape(core, (1,)), live, first, direct_lesser, flip_greater, slab, tile_cols
    )
    chips = [[2 * chip + side for chip in range(col_count // 2)] for side in range(2)]
    shares = lax.all_to_all(
        (kept + arrived).astype(jnp.bfloat16), "col", 0, 0, axis_index_groups=chips, tiled=True
    )
    scaling = 1.0 / (4.0 * math.sqrt(orbits * tile_rows * row_count))
    summed = shares.astype(jnp.float32).sum(axis=0) * scaling
    summed = summed.reshape(TW, orbits, 2, orbits).transpose(0, 2, 3, 1)
    return summed.reshape(1, TW, 2, pair_count).astype(jnp.bfloat16)


def solution(mesh):
    return jax.shard_map(
        per_device,
        mesh=mesh,
        in_specs=(P("row", "col", None, None), P("row", "col", None, None), P(), P(), P("row")),
        out_specs=P(("row", "col"), None, None, None),
        check_vma=False,
    )
```

```python
import math

import jax
import jax.numpy as jnp
from jax import lax
from jax.experimental import pallas as pl
from jax.experimental.pallas import tpu as pltpu
from jax.sharding import PartitionSpec as P

TW = 4
ORB = 64
PAIRS = 32
LANES = 128
GROUP = 4
CHIPS_Z = 4
CHIPS_X = 4


def tile_view(array):
    rows, cols, comps, pairs = array.shape
    split = array.reshape(rows, cols, comps, pairs // LANES, LANES)
    return split.transpose(0, 1, 3, 2, 4).reshape(rows * cols, comps * (pairs // LANES), LANES)


def direct_kernel(tiles_ref, swap_ref, move_ref, move_perm_ref, weight_ref, out_ref, flat, turned, turned_perm, stage, stage_perm):
    tiles = tiles_ref.shape[0]
    groups = tiles // GROUP
    flat[...] = tiles_ref[...].reshape(tiles * 2 * PAIRS, LANES).astype(jnp.float32)

    def one_group(index, carry):
        for comp in range(2):
            base = index * (GROUP * 2 * PAIRS) + comp
            block = flat[pl.ds(base, GROUP * PAIRS, stride=2), :]
            swapped = jnp.dot(
                block.astype(jnp.bfloat16), swap_ref[...], preferred_element_type=jnp.float32
            )
            turned[...] = block.T
            turned_perm[...] = swapped.T
            row = pl.multiple_of(index * (2 * PAIRS) + comp * PAIRS, PAIRS)
            for part in range(4):
                start = (part // 2) * ORB + part % 2
                cols = slice(part * LANES, (part + 1) * LANES)
                stage[pl.ds(row, PAIRS), cols] = turned[pl.ds(start, PAIRS, stride=2), :].astype(
                    jnp.bfloat16
                )
                stage_perm[pl.ds(row, PAIRS), cols] = turned_perm[
                    pl.ds(start, PAIRS, stride=2), :
                ].astype(jnp.bfloat16)
        return carry

    lax.fori_loop(0, groups, one_group, 0)
    weight = weight_ref[...]

    def one_product(index, carry):
        row = pl.multiple_of(index * (2 * PAIRS), 2 * PAIRS)
        plain = jnp.dot(
            stage[pl.ds(row, 2 * PAIRS), :], move_ref[...], preferred_element_type=jnp.float32
        )
        moved = jnp.dot(
            stage_perm[pl.ds(row, 2 * PAIRS), :],
            move_perm_ref[...],
            preferred_element_type=jnp.float32,
        )
        for item in range(GROUP):
            cols = slice(item * LANES, (item + 1) * LANES)
            a_real = plain[:PAIRS, cols]
            a_imag = plain[PAIRS:, cols]
            b_real = moved[:PAIRS, cols]
            b_imag = moved[PAIRS:, cols]
            out_ref[index * GROUP + item, 0] = weight * (a_real * b_real - a_imag * b_imag)
            out_ref[index * GROUP + item, 1] = weight * (a_real * b_imag + a_imag * b_real)
        return carry

    lax.fori_loop(0, groups, one_product, 0)


def direct_part(tiles, swap, move, move_perm, weight, block=32):
    count = tiles.shape[0]
    return pl.pallas_call(
        direct_kernel,
        grid=(count // block,),
        in_specs=[
            pl.BlockSpec((block, 2 * PAIRS, LANES), lambda n: (n, 0, 0)),
            pl.BlockSpec(swap.shape, lambda n: (0, 0)),
            pl.BlockSpec(move.shape, lambda n: (0, 0)),
            pl.BlockSpec(move_perm.shape, lambda n: (0, 0)),
            pl.BlockSpec(weight.shape, lambda n: (0, 0)),
        ],
        out_specs=pl.BlockSpec((block, 2, PAIRS, LANES), lambda n: (n, 0, 0, 0)),
        out_shape=jax.ShapeDtypeStruct((count, 2, PAIRS, LANES), jnp.float32),
        scratch_shapes=[
            pltpu.VMEM((block * 2 * PAIRS, LANES), jnp.float32),
            pltpu.VMEM((LANES, LANES), jnp.float32),
            pltpu.VMEM((LANES, LANES), jnp.float32),
            pltpu.VMEM((block // GROUP * 2 * PAIRS, GROUP * LANES), jnp.bfloat16),
            pltpu.VMEM((block // GROUP * 2 * PAIRS, GROUP * LANES), jnp.bfloat16),
        ],
        cost_estimate=pl.CostEstimate(
            flops=count * 64 * 512 * 512, bytes_accessed=count * 49152, transcendentals=0
        ),
        name="direct_part",
    )(tiles, swap, move, move_perm, weight)


def mirror_kernel(direct_ref, tiles_ref, out_ref, flat):
    tiles = tiles_ref.shape[0]
    flat[...] = tiles_ref[...].reshape(tiles * 2 * PAIRS, LANES).astype(jnp.float32)

    def one_tile(index, carry):
        m_real = flat[pl.ds(index * 2 * PAIRS, PAIRS, stride=2), :]
        m_imag = flat[pl.ds(index * 2 * PAIRS + 1, PAIRS, stride=2), :]
        d_real = direct_ref[index, 0]
        d_imag = direct_ref[index, 1]
        out_ref[index, 0] = d_real * m_real - d_imag * m_imag
        out_ref[index, 1] = d_real * m_imag + d_imag * m_real
        return carry

    lax.fori_loop(0, tiles, one_tile, 0, unroll=4)


def mirror_part(direct, tiles, block=32):
    count = tiles.shape[0]
    full = pl.BlockSpec((block, 2, PAIRS, LANES), lambda n: (n, 0, 0, 0))
    return pl.pallas_call(
        mirror_kernel,
        grid=(count // block,),
        in_specs=[full, pl.BlockSpec((block, 2 * PAIRS, LANES), lambda n: (n, 0, 0))],
        out_specs=full,
        out_shape=jax.ShapeDtypeStruct(direct.shape, jnp.float32),
        scratch_shapes=[pltpu.VMEM((block * 2 * PAIRS, LANES), jnp.float32)],
        cost_estimate=pl.CostEstimate(
            flops=count * 65536, bytes_accessed=count * 81920, transcendentals=0
        ),
        name="mirror_part",
    )(direct, tiles)


def integral_kernel(place_ref, live_ref, first_hbm, direct_hbm, tiles_hbm, slab_hbm, out_ref, first_buf, direct_buf, tiles_buf, slab_ref, flat, right, sems, slab_sem):
    number, moments, steps = tiles_buf.shape[:3]
    step = pl.program_id(0)
    slab_copy = pltpu.make_async_copy(slab_hbm, slab_ref, slab_sem)

    def copies(index):
        where = (place_ref[1] + index) % CHIPS_X
        return [
            pltpu.make_async_copy(
                source.at[:, where, place_ref[0]], target.at[index], sems.at[kind, index]
            )
            for kind, (source, target) in enumerate(
                ((tiles_hbm, tiles_buf), (first_hbm, first_buf), (direct_hbm, direct_buf))
            )
        ]

    @pl.when(step == 0)
    def _():
        for index in range(number):
            for copy in copies(index):
                copy.start()
            if index == 0:
                slab_copy.start()

    for copy in copies(step):
        copy.wait()
    first_ref = first_buf.at[step]
    direct_ref = direct_buf.at[step]
    across = (place_ref[1] + pl.program_id(0)) % CHIPS_X
    depth = steps * 2 * PAIRS
    flat[...] = tiles_buf[step].reshape(moments * depth, LANES).astype(jnp.float32)
    low = lax.broadcasted_iota(jnp.int32, (PAIRS, LANES), 1) < ORB

    def retarded(moment, item):
        time = moment * (2 * CHIPS_X) + across * 2 + place_ref[0]
        live = live_ref[time * steps + item] > 0
        base = (moment * steps + item) * 2 * PAIRS
        m_real = flat[pl.ds(base, PAIRS, stride=2), :]
        m_imag = flat[pl.ds(base + 1, PAIRS, stride=2), :]
        d_real = direct_ref[moment, item, 0]
        d_imag = direct_ref[moment, item, 1]
        ret_real = first_ref[moment, item, 0] - (d_real * m_real - d_imag * m_imag)
        ret_imag = first_ref[moment, item, 1] - (d_real * m_imag + d_imag * m_real)
        return jnp.where(live, ret_real, 0.0), jnp.where(live, ret_imag, 0.0)

    for pair in range(moments // 2):
        cols = slice(pair * LANES, (pair + 1) * LANES)
        for item in range(steps):
            left = retarded(2 * pair, item)
            other = retarded(2 * pair + 1, item)
            for comp in range(2):
                row = (item * 2 + comp) * PAIRS
                crossed = pltpu.roll(jnp.where(low, other[comp], left[comp]), ORB, 1)
                right[row : row + PAIRS, cols] = jnp.where(low, left[comp], crossed).astype(
                    jnp.bfloat16
                )
                right[depth + row : depth + row + PAIRS, cols] = jnp.where(
                    low, crossed, other[comp]
                ).astype(jnp.bfloat16)

    @pl.when(step == 0)
    def _():
        slab_copy.wait()

    product = jnp.dot(slab_ref[...], right[...], preferred_element_type=jnp.float32)
    half = product.shape[0] // 2
    lower = lax.broadcasted_iota(jnp.int32, (half, LANES), 1) < ORB
    for pair in range(moments // 2):
        cols = slice(pair * LANES, (pair + 1) * LANES)
        real = product[:half, cols]
        imag = product[half:, cols]
        crossed = pltpu.roll(jnp.where(lower, imag, real), ORB, 1)
        slot = (2 * pair + CHIPS_Z - place_ref[2]) % CHIPS_Z
        out_ref[slot] = jnp.where(lower, real, crossed)
        out_ref[(slot + 1) % CHIPS_Z] = jnp.where(lower, crossed, imag)


def integral_part(place, live, first, direct, tiles, slab, steps):
    first = first.reshape(CHIPS_Z, CHIPS_X, 2, steps, 2, PAIRS, LANES)
    direct = direct.reshape(CHIPS_Z, CHIPS_X, 2, steps, 2, PAIRS, LANES)
    tiles = tiles.reshape(CHIPS_Z, CHIPS_X, 2, steps, 2 * PAIRS, LANES)
    return pl.pallas_call(
        integral_kernel,
        grid_spec=pltpu.PrefetchScalarGridSpec(
            num_scalar_prefetch=2,
            grid=(CHIPS_X,),
            in_specs=[pl.BlockSpec(memory_space=pl.ANY)] * 4,
            out_specs=pl.BlockSpec(
                (None, CHIPS_Z, TW * ORB, LANES), lambda n, p, v: (n, 0, 0, 0)
            ),
            scratch_shapes=[
                pltpu.VMEM((CHIPS_X, CHIPS_Z, steps, 2, PAIRS, LANES), jnp.float32),
                pltpu.VMEM((CHIPS_X, CHIPS_Z, steps, 2, PAIRS, LANES), jnp.float32),
                pltpu.VMEM((CHIPS_X, CHIPS_Z, steps, 2 * PAIRS, LANES), jnp.bfloat16),
                pltpu.VMEM(slab.shape, slab.dtype),
                pltpu.VMEM((CHIPS_Z * steps * 2 * PAIRS, LANES), jnp.float32),
                pltpu.VMEM((slab.shape[1], CHIPS_Z // 2 * LANES), jnp.bfloat16),
                pltpu.SemaphoreType.DMA((3, CHIPS_X)),
                pltpu.SemaphoreType.DMA,
            ],
        ),
        out_shape=jax.ShapeDtypeStruct((CHIPS_X, CHIPS_Z, TW * ORB, LANES), jnp.float32),
        cost_estimate=pl.CostEstimate(
            flops=16 * 1024 * 512 * 128, bytes_accessed=128 * 81920, transcendentals=0
        ),
        name="integral_part",
    )(place, live, first, direct, tiles, slab)


def per_device(g_greater, g_lesser, coupling, partner, memory_start):
    tile_rows, tile_cols, components, pair_count = g_greater.shape
    row_count = lax.axis_size("row")
    col_count = lax.axis_size("col")
    orbits = coupling.shape[0]
    both = ("col", "row")
    tiles_greater = tile_view(g_greater)
    tiles_lesser = tile_view(g_lesser)
    flip_lesser = lax.all_to_all(tiles_lesser, both, 0, 0, tiled=True)

    orbit_ids = jnp.arange(orbits, dtype=jnp.int32)
    one_hot = (partner[:, None] == orbit_ids[None, :]).astype(jnp.bfloat16)
    swap = jnp.kron(jnp.eye(2, dtype=jnp.bfloat16), one_hot.T)
    source = jnp.arange(GROUP * LANES, dtype=jnp.int32)
    src_ib = source // (2 * LANES)
    src_jb = source // LANES % 2
    src_item = source % LANES // PAIRS
    src_orbit = source % PAIRS * 2 + src_ib
    dst_item = source // LANES
    dst_jb = source // ORB % 2
    dst_orbit = source % ORB
    same = (src_item[:, None] == dst_item[None, :]) & (src_jb[:, None] == dst_jb[None, :])
    move = (same & (src_orbit[:, None] == dst_orbit[None, :])).astype(jnp.bfloat16)
    wanted = jnp.tile(partner, 2 * GROUP)
    move_perm = (same & (src_orbit[:, None] == wanted[None, :])).astype(jnp.bfloat16)
    weight = coupling.T.reshape(PAIRS, LANES)

    direct_lesser = direct_part(tiles_lesser, swap, move, move_perm, weight)
    direct_greater = direct_part(tiles_greater, swap, move, move_perm, weight)
    tiles_greater, direct_lesser, direct_greater = lax.optimization_barrier(
        (tiles_greater, direct_lesser, direct_greater)
    )
    flip_greater = lax.all_to_all(tiles_greater, both, 0, 0, tiled=True)
    first = mirror_part(direct_greater, flip_lesser)

    window = flip_lesser[: TW * tile_cols].reshape(TW, tile_cols, PAIRS, 2, 2, orbits)
    slab_real = window[:, :, :, 0]
    slab_imag = window[:, :, :, 1]
    to_real = jnp.stack([slab_real, -slab_imag], axis=0)
    to_imag = jnp.stack([slab_imag, slab_real], axis=0)
    slab = jnp.stack([to_real, to_imag], axis=0)
    slab = slab.transpose(0, 2, 6, 5, 3, 1, 4).reshape(
        2 * TW * orbits, 2 * tile_cols * 2 * PAIRS
    )
    first_times = lax.axis_index("row") * tile_rows + jnp.arange(tile_rows, dtype=jnp.int32)
    second_times = jnp.arange(tile_cols, dtype=jnp.int32) * col_count + lax.axis_index("col")
    live = (second_times[None, :] >= memory_start[:, None]) & (
        second_times[None, :] <= first_times[:, None]
    )
    live = live.astype(jnp.int32).reshape(tile_rows * tile_cols)
    column = lax.axis_index("col")
    core = column % 2
    along = column // 2 % CHIPS_X
    depth = column // (2 * CHIPS_X)
    away = integral_part(
        jnp.stack([1 - core, along, depth]), live, first, direct_lesser, flip_greater, slab, tile_cols
    )
    arrived = lax.ppermute(away, "col", [(item, item ^ 1) for item in range(col_count)])
    kept = integral_part(
        jnp.stack([core, along, depth]), live, first, direct_lesser, flip_greater, slab, tile_cols
    )
    places = [
        (z, x, side) for z in range(CHIPS_Z) for x in range(CHIPS_X) for side in range(2)
    ]

    def name_of(z, x, side):
        return (z % CHIPS_Z * CHIPS_X + x % CHIPS_X) * 2 + side

    summed = kept[0] + arrived[0]
    parts = [
        lax.ppermute(
            (kept[shift] + arrived[shift]).astype(jnp.bfloat16),
            "col",
            [(name_of(z, x, side), name_of(z, x + shift, side)) for z, x, side in places],
        )
        for shift in range(1, CHIPS_X)
    ]
    for part in parts:
        summed = summed + part.astype(jnp.float32)
    total = summed[0]
    parts = [
        lax.ppermute(
            summed[shift].astype(jnp.bfloat16),
            "col",
            [(name_of(z, x, side), name_of(z + shift, x, side)) for z, x, side in places],
        )
        for shift in range(1, CHIPS_Z)
    ]
    for part in parts:
        total = total + part.astype(jnp.float32)
    scaling = 1.0 / (4.0 * math.sqrt(orbits * tile_rows * row_count))
    total = total * scaling
    total = total.reshape(TW, orbits, 2, orbits).transpose(0, 2, 3, 1)
    return total.reshape(1, TW, 2, pair_count).astype(jnp.bfloat16)


def solution(mesh):
    return jax.shard_map(
        per_device,
        mesh=mesh,
        in_specs=(P("row", "col", None, None), P("row", "col", None, None), P(), P(), P("row")),
        out_specs=P(("row", "col"), None, None, None),
        check_vma=False,
    )
```

```python
import math

import jax
import jax.numpy as jnp
from jax import lax
from jax.experimental import pallas as pl
from jax.experimental.pallas import tpu as pltpu
from jax.sharding import PartitionSpec as P

TW = 4
ORB = 64
PAIRS = 32
LANES = 128
GROUP = 4
CHIPS_Z = 4
CHIPS_X = 4
INTEGRAL_VMEM = 44 * 1024 * 1024


def tile_view(array):
    rows, cols, comps, pairs = array.shape
    split = array.reshape(rows, cols, comps, pairs // LANES, LANES)
    return split.transpose(0, 1, 3, 2, 4).reshape(rows * cols, comps * (pairs // LANES), LANES)


def direct_kernel(live_ref, tiles_ref, swap_ref, move_ref, move_perm_ref, weight_ref, out_ref, flat, turned, turned_perm, stage, stage_perm):
    tiles = tiles_ref.shape[0]
    groups = tiles // GROUP
    flat[...] = tiles_ref[...].reshape(tiles * 2 * PAIRS, LANES).astype(jnp.float32)

    def one_group(index, carry):
        for comp in range(2):
            base = index * (GROUP * 2 * PAIRS) + comp
            block = flat[pl.ds(base, GROUP * PAIRS, stride=2), :]
            swapped = jnp.dot(
                block.astype(jnp.bfloat16), swap_ref[...], preferred_element_type=jnp.float32
            )
            turned[...] = block.T
            turned_perm[...] = swapped.T
            row = pl.multiple_of(index * (2 * PAIRS) + comp * PAIRS, PAIRS)
            for part in range(4):
                start = (part // 2) * ORB + part % 2
                cols = slice(part * LANES, (part + 1) * LANES)
                stage[pl.ds(row, PAIRS), cols] = turned[pl.ds(start, PAIRS, stride=2), :].astype(
                    jnp.bfloat16
                )
                stage_perm[pl.ds(row, PAIRS), cols] = turned_perm[
                    pl.ds(start, PAIRS, stride=2), :
                ].astype(jnp.bfloat16)
        return carry

    lax.fori_loop(0, groups, one_group, 0)
    weight = weight_ref[...]

    def one_product(index, carry):
        row = pl.multiple_of(index * (2 * PAIRS), 2 * PAIRS)
        plain = jnp.dot(
            stage[pl.ds(row, 2 * PAIRS), :], move_ref[...], preferred_element_type=jnp.float32
        )
        moved = jnp.dot(
            stage_perm[pl.ds(row, 2 * PAIRS), :],
            move_perm_ref[...],
            preferred_element_type=jnp.float32,
        )
        for item in range(GROUP):
            cols = slice(item * LANES, (item + 1) * LANES)
            live = live_ref[pl.program_id(0) * tiles + index * GROUP + item] > 0
            kept = jnp.where(live, weight, 0.0)
            a_real = plain[:PAIRS, cols]
            a_imag = plain[PAIRS:, cols]
            b_real = moved[:PAIRS, cols]
            b_imag = moved[PAIRS:, cols]
            out_ref[index * GROUP + item, 0] = kept * (a_real * b_real - a_imag * b_imag)
            out_ref[index * GROUP + item, 1] = kept * (a_real * b_imag + a_imag * b_real)
        return carry

    lax.fori_loop(0, groups, one_product, 0)


def direct_part(live, tiles, swap, move, move_perm, weight, block=32):
    count = tiles.shape[0]
    return pl.pallas_call(
        direct_kernel,
        grid=(count // block,),
        in_specs=[
            pl.BlockSpec(memory_space=pltpu.SMEM),
            pl.BlockSpec((block, 2 * PAIRS, LANES), lambda n: (n, 0, 0)),
            pl.BlockSpec(swap.shape, lambda n: (0, 0)),
            pl.BlockSpec(move.shape, lambda n: (0, 0)),
            pl.BlockSpec(move_perm.shape, lambda n: (0, 0)),
            pl.BlockSpec(weight.shape, lambda n: (0, 0)),
        ],
        out_specs=pl.BlockSpec((block, 2, PAIRS, LANES), lambda n: (n, 0, 0, 0)),
        out_shape=jax.ShapeDtypeStruct((count, 2, PAIRS, LANES), jnp.float32),
        scratch_shapes=[
            pltpu.VMEM((block * 2 * PAIRS, LANES), jnp.float32),
            pltpu.VMEM((LANES, LANES), jnp.float32),
            pltpu.VMEM((LANES, LANES), jnp.float32),
            pltpu.VMEM((block // GROUP * 2 * PAIRS, GROUP * LANES), jnp.bfloat16),
            pltpu.VMEM((block // GROUP * 2 * PAIRS, GROUP * LANES), jnp.bfloat16),
        ],
        cost_estimate=pl.CostEstimate(
            flops=count * 64 * 512 * 512, bytes_accessed=count * 49152, transcendentals=0
        ),
        name="direct_part",
    )(live, tiles, swap, move, move_perm, weight)


def mirror_kernel(direct_ref, tiles_ref, out_ref, flat):
    tiles = tiles_ref.shape[0]
    flat[...] = tiles_ref[...].reshape(tiles * 2 * PAIRS, LANES).astype(jnp.float32)

    def one_tile(index, carry):
        m_real = flat[pl.ds(index * 2 * PAIRS, PAIRS, stride=2), :]
        m_imag = flat[pl.ds(index * 2 * PAIRS + 1, PAIRS, stride=2), :]
        d_real = direct_ref[index, 0]
        d_imag = direct_ref[index, 1]
        out_ref[index, 0] = d_real * m_real - d_imag * m_imag
        out_ref[index, 1] = d_real * m_imag + d_imag * m_real
        return carry

    lax.fori_loop(0, tiles, one_tile, 0, unroll=4)


def mirror_part(direct, tiles, block=32):
    count = tiles.shape[0]
    full = pl.BlockSpec((block, 2, PAIRS, LANES), lambda n: (n, 0, 0, 0))
    return pl.pallas_call(
        mirror_kernel,
        grid=(count // block,),
        in_specs=[full, pl.BlockSpec((block, 2 * PAIRS, LANES), lambda n: (n, 0, 0))],
        out_specs=full,
        out_shape=jax.ShapeDtypeStruct(direct.shape, jnp.float32),
        scratch_shapes=[pltpu.VMEM((block * 2 * PAIRS, LANES), jnp.float32)],
        cost_estimate=pl.CostEstimate(
            flops=count * 65536, bytes_accessed=count * 81920, transcendentals=0
        ),
        name="mirror_part",
    )(direct, tiles)


def integral_kernel(place_ref, first_ref, direct_ref, tiles_ref, slab_ref, out_ref, flat, right):
    moments, steps = tiles_ref.shape[:2]
    depth = steps * 2 * PAIRS
    flat[...] = tiles_ref[...].reshape(moments * depth, LANES).astype(jnp.float32)
    low = lax.broadcasted_iota(jnp.int32, (PAIRS, LANES), 1) < ORB

    def retarded(moment, item):
        base = (moment * steps + item) * 2 * PAIRS
        m_real = flat[pl.ds(base, PAIRS, stride=2), :]
        m_imag = flat[pl.ds(base + 1, PAIRS, stride=2), :]
        d_real = direct_ref[moment, item, 0]
        d_imag = direct_ref[moment, item, 1]
        ret_real = first_ref[moment, item, 0] - (d_real * m_real - d_imag * m_imag)
        ret_imag = first_ref[moment, item, 1] - (d_real * m_imag + d_imag * m_real)
        return ret_real, ret_imag

    for pair in range(moments // 2):
        cols = slice(pair * LANES, (pair + 1) * LANES)
        for item in range(steps):
            left = retarded(2 * pair, item)
            other = retarded(2 * pair + 1, item)
            for comp in range(2):
                row = (item * 2 + comp) * PAIRS
                right[row : row + PAIRS, cols] = jnp.where(
                    low, left[comp], pltpu.roll(other[comp], ORB, 1)
                ).astype(jnp.bfloat16)
                right[depth + row : depth + row + PAIRS, cols] = jnp.where(
                    low, pltpu.roll(left[comp], ORB, 1), other[comp]
                ).astype(jnp.bfloat16)
    product = jnp.dot(slab_ref[...], right[...], preferred_element_type=jnp.float32)
    half = product.shape[0] // 2
    lower = lax.broadcasted_iota(jnp.int32, (half, LANES), 1) < ORB
    for pair in range(moments // 2):
        cols = slice(pair * LANES, (pair + 1) * LANES)
        real = product[:half, cols]
        imag = product[half:, cols]
        crossed = pltpu.roll(jnp.where(lower, imag, real), ORB, 1)
        slot = (2 * pair + CHIPS_Z - place_ref[2]) % CHIPS_Z
        out_ref[slot] = jnp.where(lower, real, crossed)
        out_ref[(slot + 1) % CHIPS_Z] = jnp.where(lower, crossed, imag)


def integral_part(place, first, direct, tiles, slab, steps):
    first = first.reshape(CHIPS_Z, CHIPS_X, 2, steps, 2, PAIRS, LANES)
    direct = direct.reshape(CHIPS_Z, CHIPS_X, 2, steps, 2, PAIRS, LANES)
    tiles = tiles.reshape(CHIPS_Z, CHIPS_X, 2, steps, 2 * PAIRS, LANES)
    full = pl.BlockSpec(
        (CHIPS_Z, None, None, steps, 2, PAIRS, LANES),
        lambda n, p: (0, (p[1] + n) % CHIPS_X, p[0], 0, 0, 0, 0),
    )
    return pl.pallas_call(
        integral_kernel,
        grid_spec=pltpu.PrefetchScalarGridSpec(
            num_scalar_prefetch=1,
            grid=(CHIPS_X,),
            in_specs=[
                full,
                full,
                pl.BlockSpec(
                    (CHIPS_Z, None, None, steps, 2 * PAIRS, LANES),
                    lambda n, p: (0, (p[1] + n) % CHIPS_X, p[0], 0, 0, 0),
                ),
                pl.BlockSpec(slab.shape, lambda n, p: (0, 0)),
            ],
            out_specs=pl.BlockSpec(
                (None, CHIPS_Z, TW * ORB, LANES), lambda n, p: (n, 0, 0, 0)
            ),
            scratch_shapes=[
                pltpu.VMEM((CHIPS_Z * steps * 2 * PAIRS, LANES), jnp.float32),
                pltpu.VMEM((slab.shape[1], CHIPS_Z // 2 * LANES), jnp.bfloat16),
            ],
        ),
        out_shape=jax.ShapeDtypeStruct((CHIPS_X, CHIPS_Z, TW * ORB, LANES), jnp.float32),
        cost_estimate=pl.CostEstimate(
            flops=16 * 1024 * 512 * 128, bytes_accessed=128 * 81920, transcendentals=0
        ),
        compiler_params=pltpu.CompilerParams(vmem_limit_bytes=INTEGRAL_VMEM),
        name="integral_part",
    )(place, first, direct, tiles, slab)


def per_device(g_greater, g_lesser, coupling, partner, memory_start):
    tile_rows, tile_cols, components, pair_count = g_greater.shape
    row_count = lax.axis_size("row")
    col_count = lax.axis_size("col")
    orbits = coupling.shape[0]
    both = ("col", "row")
    tiles_greater = tile_view(g_greater)
    tiles_lesser = tile_view(g_lesser)
    flip_lesser = lax.all_to_all(tiles_lesser, both, 0, 0, tiled=True)

    orbit_ids = jnp.arange(orbits, dtype=jnp.int32)
    one_hot = (partner[:, None] == orbit_ids[None, :]).astype(jnp.bfloat16)
    swap = jnp.kron(jnp.eye(2, dtype=jnp.bfloat16), one_hot.T)
    source = jnp.arange(GROUP * LANES, dtype=jnp.int32)
    src_ib = source // (2 * LANES)
    src_jb = source // LANES % 2
    src_item = source % LANES // PAIRS
    src_orbit = source % PAIRS * 2 + src_ib
    dst_item = source // LANES
    dst_jb = source // ORB % 2
    dst_orbit = source % ORB
    same = (src_item[:, None] == dst_item[None, :]) & (src_jb[:, None] == dst_jb[None, :])
    move = (same & (src_orbit[:, None] == dst_orbit[None, :])).astype(jnp.bfloat16)
    wanted = jnp.tile(partner, 2 * GROUP)
    move_perm = (same & (src_orbit[:, None] == wanted[None, :])).astype(jnp.bfloat16)
    weight = coupling.T.reshape(PAIRS, LANES)

    first_times = lax.axis_index("row") * tile_rows + jnp.arange(tile_rows, dtype=jnp.int32)
    second_times = jnp.arange(tile_cols, dtype=jnp.int32) * col_count + lax.axis_index("col")
    live = (second_times[None, :] >= memory_start[:, None]) & (
        second_times[None, :] <= first_times[:, None]
    )
    live = live.astype(jnp.int32).reshape(tile_rows * tile_cols)
    column = lax.axis_index("col")
    core = column % 2
    along = column // 2 % CHIPS_X
    depth = column // (2 * CHIPS_X)
    place_away = jnp.stack([1 - core, along, depth])
    place_kept = jnp.stack([core, along, depth])

    direct_lesser = direct_part(live, tiles_lesser, swap, move, move_perm, weight)
    direct_greater = direct_part(live, tiles_greater, swap, move, move_perm, weight)
    tiles_greater, direct_lesser, direct_greater, place_away, place_kept = lax.optimization_barrier(
        (tiles_greater, direct_lesser, direct_greater, place_away, place_kept)
    )
    flip_greater = lax.all_to_all(tiles_greater, both, 0, 0, tiled=True)
    first = mirror_part(direct_greater, flip_lesser)

    window = flip_lesser[: TW * tile_cols].reshape(TW, tile_cols, PAIRS, 2, 2, orbits)
    slab_real = window[:, :, :, 0]
    slab_imag = window[:, :, :, 1]
    to_real = jnp.stack([slab_real, -slab_imag], axis=0)
    to_imag = jnp.stack([slab_imag, slab_real], axis=0)
    slab = jnp.stack([to_real, to_imag], axis=0)
    slab = slab.transpose(0, 2, 6, 5, 3, 1, 4).reshape(
        2 * TW * orbits, 2 * tile_cols * 2 * PAIRS
    )
    away = integral_part(
        place_away, first, direct_lesser, flip_greater, slab, tile_cols
    )
    arrived = lax.ppermute(away, "col", [(item, item ^ 1) for item in range(col_count)])
    kept = integral_part(
        place_kept, first, direct_lesser, flip_greater, slab, tile_cols
    )
    places = [
        (z, x, side) for z in range(CHIPS_Z) for x in range(CHIPS_X) for side in range(2)
    ]

    def name_of(z, x, side):
        return (z % CHIPS_Z * CHIPS_X + x % CHIPS_X) * 2 + side

    summed = kept[0] + arrived[0]
    parts = [
        lax.ppermute(
            (kept[shift] + arrived[shift]).astype(jnp.bfloat16),
            "col",
            [(name_of(z, x, side), name_of(z, x + shift, side)) for z, x, side in places],
        )
        for shift in range(1, CHIPS_X)
    ]
    for part in parts:
        summed = summed + part.astype(jnp.float32)
    total = summed[0]
    parts = [
        lax.ppermute(
            summed[shift].astype(jnp.bfloat16),
            "col",
            [(name_of(z, x, side), name_of(z + shift, x, side)) for z, x, side in places],
        )
        for shift in range(1, CHIPS_Z)
    ]
    for part in parts:
        total = total + part.astype(jnp.float32)
    scaling = 1.0 / (4.0 * math.sqrt(orbits * tile_rows * row_count))
    total = total * scaling
    total = total.reshape(TW, orbits, 2, orbits).transpose(0, 2, 3, 1)
    return total.reshape(1, TW, 2, pair_count).astype(jnp.bfloat16)


def solution(mesh):
    return jax.shard_map(
        per_device,
        mesh=mesh,
        in_specs=(P("row", "col", None, None), P("row", "col", None, None), P(), P(), P("row")),
        out_specs=P(("row", "col"), None, None, None),
        check_vma=False,
    )
```

```python
import math

import jax
import jax.numpy as jnp
from jax import lax
from jax.experimental import pallas as pl
from jax.experimental.pallas import tpu as pltpu
from jax.sharding import PartitionSpec as P

TW = 4
ORB = 64
PAIRS = 32
LANES = 128
GROUP = 4
CHIPS_Z = 4
CHIPS_X = 4
INTEGRAL_VMEM = 48 * 1024 * 1024


def tile_view(array):
    rows, cols, comps, pairs = array.shape
    split = array.reshape(rows, cols, comps, pairs // LANES, LANES)
    return split.transpose(0, 1, 3, 2, 4).reshape(rows * cols, comps * (pairs // LANES), LANES)


def direct_kernel(live_ref, tiles_ref, swap_ref, move_ref, move_perm_ref, weight_ref, out_ref, flat, turned, turned_perm, stage, stage_perm):
    tiles = tiles_ref.shape[0]
    groups = tiles // GROUP
    flat[...] = tiles_ref[...].reshape(tiles * 2 * PAIRS, LANES).astype(jnp.float32)

    def one_group(index, carry):
        for comp in range(2):
            base = index * (GROUP * 2 * PAIRS) + comp
            block = flat[pl.ds(base, GROUP * PAIRS, stride=2), :]
            swapped = jnp.dot(
                block.astype(jnp.bfloat16), swap_ref[...], preferred_element_type=jnp.float32
            )
            turned[...] = block.T
            turned_perm[...] = swapped.T
            row = pl.multiple_of(index * (2 * PAIRS) + comp * PAIRS, PAIRS)
            for part in range(4):
                start = (part // 2) * ORB + part % 2
                cols = slice(part * LANES, (part + 1) * LANES)
                stage[pl.ds(row, PAIRS), cols] = turned[pl.ds(start, PAIRS, stride=2), :].astype(
                    jnp.bfloat16
                )
                stage_perm[pl.ds(row, PAIRS), cols] = turned_perm[
                    pl.ds(start, PAIRS, stride=2), :
                ].astype(jnp.bfloat16)
        return carry

    lax.fori_loop(0, groups, one_group, 0)
    weight = weight_ref[...]

    def one_product(index, carry):
        row = pl.multiple_of(index * (2 * PAIRS), 2 * PAIRS)
        plain = jnp.dot(
            stage[pl.ds(row, 2 * PAIRS), :], move_ref[...], preferred_element_type=jnp.float32
        )
        moved = jnp.dot(
            stage_perm[pl.ds(row, 2 * PAIRS), :],
            move_perm_ref[...],
            preferred_element_type=jnp.float32,
        )
        for item in range(GROUP):
            cols = slice(item * LANES, (item + 1) * LANES)
            live = live_ref[pl.program_id(0) * tiles + index * GROUP + item] > 0
            kept = jnp.where(live, weight, 0.0)
            a_real = plain[:PAIRS, cols]
            a_imag = plain[PAIRS:, cols]
            b_real = moved[:PAIRS, cols]
            b_imag = moved[PAIRS:, cols]
            out_ref[index * GROUP + item, 0] = kept * (a_real * b_real - a_imag * b_imag)
            out_ref[index * GROUP + item, 1] = kept * (a_real * b_imag + a_imag * b_real)
        return carry

    lax.fori_loop(0, groups, one_product, 0)


def direct_part(live, tiles, swap, move, move_perm, weight, block=32):
    count = tiles.shape[0]
    return pl.pallas_call(
        direct_kernel,
        grid=(count // block,),
        in_specs=[
            pl.BlockSpec(memory_space=pltpu.SMEM),
            pl.BlockSpec((block, 2 * PAIRS, LANES), lambda n: (n, 0, 0)),
            pl.BlockSpec(swap.shape, lambda n: (0, 0)),
            pl.BlockSpec(move.shape, lambda n: (0, 0)),
            pl.BlockSpec(move_perm.shape, lambda n: (0, 0)),
            pl.BlockSpec(weight.shape, lambda n: (0, 0)),
        ],
        out_specs=pl.BlockSpec((block, 2, PAIRS, LANES), lambda n: (n, 0, 0, 0)),
        out_shape=jax.ShapeDtypeStruct((count, 2, PAIRS, LANES), jnp.float32),
        scratch_shapes=[
            pltpu.VMEM((block * 2 * PAIRS, LANES), jnp.float32),
            pltpu.VMEM((LANES, LANES), jnp.float32),
            pltpu.VMEM((LANES, LANES), jnp.float32),
            pltpu.VMEM((block // GROUP * 2 * PAIRS, GROUP * LANES), jnp.bfloat16),
            pltpu.VMEM((block // GROUP * 2 * PAIRS, GROUP * LANES), jnp.bfloat16),
        ],
        cost_estimate=pl.CostEstimate(
            flops=count * 64 * 512 * 512, bytes_accessed=count * 49152, transcendentals=0
        ),
        name="direct_part",
    )(live, tiles, swap, move, move_perm, weight)


def mirror_kernel(direct_ref, tiles_ref, out_ref, flat):
    tiles = tiles_ref.shape[0]
    flat[...] = tiles_ref[...].reshape(tiles * 2 * PAIRS, LANES).astype(jnp.float32)

    def one_tile(index, carry):
        m_real = flat[pl.ds(index * 2 * PAIRS, PAIRS, stride=2), :]
        m_imag = flat[pl.ds(index * 2 * PAIRS + 1, PAIRS, stride=2), :]
        d_real = direct_ref[index, 0]
        d_imag = direct_ref[index, 1]
        out_ref[index, 0] = d_real * m_real - d_imag * m_imag
        out_ref[index, 1] = d_real * m_imag + d_imag * m_real
        return carry

    lax.fori_loop(0, tiles, one_tile, 0, unroll=4)


def mirror_part(direct, tiles, block=32):
    count = tiles.shape[0]
    full = pl.BlockSpec((block, 2, PAIRS, LANES), lambda n: (n, 0, 0, 0))
    return pl.pallas_call(
        mirror_kernel,
        grid=(count // block,),
        in_specs=[full, pl.BlockSpec((block, 2 * PAIRS, LANES), lambda n: (n, 0, 0))],
        out_specs=full,
        out_shape=jax.ShapeDtypeStruct(direct.shape, jnp.float32),
        scratch_shapes=[pltpu.VMEM((block * 2 * PAIRS, LANES), jnp.float32)],
        cost_estimate=pl.CostEstimate(
            flops=count * 65536, bytes_accessed=count * 81920, transcendentals=0
        ),
        name="mirror_part",
    )(direct, tiles)


def integral_kernel(place_ref, first_ref, direct_ref, tiles_ref, slab_ref, out_ref, flat, right):
    moments, steps = tiles_ref.shape[:2]
    depth = steps * 2 * PAIRS
    flat[...] = tiles_ref[...].reshape(moments * depth, LANES).astype(jnp.float32)
    low = lax.broadcasted_iota(jnp.int32, (PAIRS, LANES), 1) < ORB

    def retarded(moment, item):
        base = (moment * steps + item) * 2 * PAIRS
        m_real = flat[pl.ds(base, PAIRS, stride=2), :]
        m_imag = flat[pl.ds(base + 1, PAIRS, stride=2), :]
        d_real = direct_ref[moment, item, 0]
        d_imag = direct_ref[moment, item, 1]
        ret_real = first_ref[moment, item, 0] - (d_real * m_real - d_imag * m_imag)
        ret_imag = first_ref[moment, item, 1] - (d_real * m_imag + d_imag * m_real)
        return ret_real, ret_imag

    for pair in range(moments // 2):
        cols = slice(pair * LANES, (pair + 1) * LANES)
        for item in range(steps):
            left = retarded(2 * pair, item)
            other = retarded(2 * pair + 1, item)
            for comp in range(2):
                row = (item * 2 + comp) * PAIRS
                right[row : row + PAIRS, cols] = jnp.where(
                    low, left[comp], pltpu.roll(other[comp], ORB, 1)
                ).astype(jnp.bfloat16)
                right[depth + row : depth + row + PAIRS, cols] = jnp.where(
                    low, pltpu.roll(left[comp], ORB, 1), other[comp]
                ).astype(jnp.bfloat16)
    product = jnp.dot(slab_ref[...], right[...], preferred_element_type=jnp.float32)
    half = product.shape[0] // 2
    lower = lax.broadcasted_iota(jnp.int32, (half, LANES), 1) < ORB
    for pair in range(moments // 2):
        cols = slice(pair * LANES, (pair + 1) * LANES)
        real = product[:half, cols]
        imag = product[half:, cols]
        crossed = pltpu.roll(jnp.where(lower, imag, real), ORB, 1)
        slot = (2 * pair + CHIPS_Z - place_ref[2]) % CHIPS_Z
        out_ref[slot] = jnp.where(lower, real, crossed)
        out_ref[(slot + 1) % CHIPS_Z] = jnp.where(lower, crossed, imag)


def integral_part(place, first, direct, tiles, slab, steps):
    first = first.reshape(CHIPS_Z, CHIPS_X, 2, steps, 2, PAIRS, LANES)
    direct = direct.reshape(CHIPS_Z, CHIPS_X, 2, steps, 2, PAIRS, LANES)
    tiles = tiles.reshape(CHIPS_Z, CHIPS_X, 2, steps, 2 * PAIRS, LANES)
    full = pl.BlockSpec(
        (CHIPS_Z, None, None, steps, 2, PAIRS, LANES),
        lambda n, p: (0, (p[1] + n) % CHIPS_X, p[0], 0, 0, 0, 0),
    )
    return pl.pallas_call(
        integral_kernel,
        grid_spec=pltpu.PrefetchScalarGridSpec(
            num_scalar_prefetch=1,
            grid=(CHIPS_X,),
            in_specs=[
                full,
                full,
                pl.BlockSpec(
                    (CHIPS_Z, None, None, steps, 2 * PAIRS, LANES),
                    lambda n, p: (0, (p[1] + n) % CHIPS_X, p[0], 0, 0, 0),
                ),
                pl.BlockSpec(slab.shape, lambda n, p: (0, 0)),
            ],
            out_specs=pl.BlockSpec(
                (None, CHIPS_Z, TW * ORB, LANES), lambda n, p: (n, 0, 0, 0)
            ),
            scratch_shapes=[
                pltpu.VMEM((CHIPS_Z * steps * 2 * PAIRS, LANES), jnp.float32),
                pltpu.VMEM((slab.shape[1], CHIPS_Z // 2 * LANES), jnp.bfloat16),
            ],
        ),
        out_shape=jax.ShapeDtypeStruct((CHIPS_X, CHIPS_Z, TW * ORB, LANES), jnp.float32),
        cost_estimate=pl.CostEstimate(
            flops=16 * 1024 * 512 * 128, bytes_accessed=128 * 81920, transcendentals=0
        ),
        compiler_params=pltpu.CompilerParams(vmem_limit_bytes=INTEGRAL_VMEM),
        name="integral_part",
    )(place, first, direct, tiles, slab)


def per_device(g_greater, g_lesser, coupling, partner, memory_start):
    tile_rows, tile_cols, components, pair_count = g_greater.shape
    row_count = lax.axis_size("row")
    col_count = lax.axis_size("col")
    orbits = coupling.shape[0]
    both = ("col", "row")
    tiles_greater = tile_view(g_greater)
    tiles_lesser = tile_view(g_lesser)
    flip_lesser = lax.all_to_all(tiles_lesser, both, 0, 0, tiled=True)

    orbit_ids = jnp.arange(orbits, dtype=jnp.int32)
    one_hot = (partner[:, None] == orbit_ids[None, :]).astype(jnp.bfloat16)
    swap = jnp.kron(jnp.eye(2, dtype=jnp.bfloat16), one_hot.T)
    source = jnp.arange(GROUP * LANES, dtype=jnp.int32)
    src_ib = source // (2 * LANES)
    src_jb = source // LANES % 2
    src_item = source % LANES // PAIRS
    src_orbit = source % PAIRS * 2 + src_ib
    dst_item = source // LANES
    dst_jb = source // ORB % 2
    dst_orbit = source % ORB
    same = (src_item[:, None] == dst_item[None, :]) & (src_jb[:, None] == dst_jb[None, :])
    move = (same & (src_orbit[:, None] == dst_orbit[None, :])).astype(jnp.bfloat16)
    wanted = jnp.tile(partner, 2 * GROUP)
    move_perm = (same & (src_orbit[:, None] == wanted[None, :])).astype(jnp.bfloat16)
    weight = coupling.T.reshape(PAIRS, LANES)

    first_times = lax.axis_index("row") * tile_rows + jnp.arange(tile_rows, dtype=jnp.int32)
    second_times = jnp.arange(tile_cols, dtype=jnp.int32) * col_count + lax.axis_index("col")
    live = (second_times[None, :] >= memory_start[:, None]) & (
        second_times[None, :] <= first_times[:, None]
    )
    live = live.astype(jnp.int32).reshape(tile_rows * tile_cols)
    column = lax.axis_index("col")
    core = column % 2
    along = column // 2 % CHIPS_X
    depth = column // (2 * CHIPS_X)
    place_away = jnp.stack([1 - core, along, depth])
    place_kept = jnp.stack([core, along, depth])

    direct_lesser = direct_part(live, tiles_lesser, swap, move, move_perm, weight)
    direct_greater = direct_part(live, tiles_greater, swap, move, move_perm, weight)
    tiles_greater, direct_lesser, direct_greater, place_away, place_kept = lax.optimization_barrier(
        (tiles_greater, direct_lesser, direct_greater, place_away, place_kept)
    )
    flip_greater = lax.all_to_all(tiles_greater, both, 0, 0, tiled=True)
    first = mirror_part(direct_greater, flip_lesser)

    window = flip_lesser[: TW * tile_cols].reshape(TW, tile_cols, PAIRS, 2, 2, orbits)
    slab_real = window[:, :, :, 0]
    slab_imag = window[:, :, :, 1]
    to_real = jnp.stack([slab_real, -slab_imag], axis=0)
    to_imag = jnp.stack([slab_imag, slab_real], axis=0)
    slab = jnp.stack([to_real, to_imag], axis=0)
    slab = slab.transpose(0, 2, 6, 5, 3, 1, 4).reshape(
        2 * TW * orbits, 2 * tile_cols * 2 * PAIRS
    )
    away = integral_part(
        place_away, first, direct_lesser, flip_greater, slab, tile_cols
    )
    arrived = lax.ppermute(away, "col", [(item, item ^ 1) for item in range(col_count)])
    kept = integral_part(
        place_kept, first, direct_lesser, flip_greater, slab, tile_cols
    )
    places = [
        (z, x, side) for z in range(CHIPS_Z) for x in range(CHIPS_X) for side in range(2)
    ]

    def name_of(z, x, side):
        return (z % CHIPS_Z * CHIPS_X + x % CHIPS_X) * 2 + side

    summed = kept[0] + arrived[0]
    parts = [
        lax.ppermute(
            (kept[shift] + arrived[shift]).astype(jnp.bfloat16),
            "col",
            [(name_of(z, x, side), name_of(z, x + shift, side)) for z, x, side in places],
        )
        for shift in (2, 1, 3)
    ]
    for part in parts:
        summed = summed + part.astype(jnp.float32)
    total = summed[0]
    parts = [
        lax.ppermute(
            summed[shift].astype(jnp.bfloat16),
            "col",
            [(name_of(z, x, side), name_of(z + shift, x, side)) for z, x, side in places],
        )
        for shift in range(1, CHIPS_Z)
    ]
    for part in parts:
        total = total + part.astype(jnp.float32)
    scaling = 1.0 / (4.0 * math.sqrt(orbits * tile_rows * row_count))
    total = total * scaling
    total = total.reshape(TW, orbits, 2, orbits).transpose(0, 2, 3, 1)
    return total.reshape(1, TW, 2, pair_count).astype(jnp.bfloat16)


def solution(mesh):
    return jax.shard_map(
        per_device,
        mesh=mesh,
        in_specs=(P("row", "col", None, None), P("row", "col", None, None), P(), P(), P("row")),
        out_specs=P(("row", "col"), None, None, None),
        check_vma=False,
    )
```
